128 devices in a mesh: gx: 8 (over x, y_hi), gy: 16 (over z, y_lo, core).
Axes of the slice: x: 4, y: 4 (y_hi: 2, y_lo: 2; y = y_hi * 2 + y_lo), z: 4, core: 2. Of those that a mesh axis runs over, the one named last changes fastest.
Arguments:
- u_wind: float32 [64, 128, 2048], P(None, 'gx', 'gy'), may hold values from -6 to 6
- v_wind: float32 [64, 128, 2048], P(None, 'gx', 'gy'), may hold values from -6 to 6
- w_wind: float32 [64, 128, 2048], P(None, 'gx', 'gy'), may hold values from -4 to 4
- pressure: float32 [64, 128, 2048], P(None, 'gx', 'gy'), may hold values from -6 to 6
- terrain_level: int32 [128, 2048], P('gx', 'gy'), may hold values from 0 to 8
- zone_width: int32 [4], replicated, may hold values from 5 to 16
- stiffness: float32 [64], replicated, may hold values from 0.25 to 2
- inflow_profile: float32 [2, 64], replicated, may hold values from -5 to 5
Outputs:
- u_final: float32 [64, 128, 2048], P(None, 'gx', 'gy')
- v_final: float32 [64, 128, 2048], P(None, 'gx', 'gy')
- w_final: float32 [64, 128, 2048], P(None, 'gx', 'gy')
- p_final: float32 [64, 128, 2048], P(None, 'gx', 'gy')
The draws below stay inside these ranges and needn't reach their ends.
Inputs may be any that keep to these rules, and one draw needn't show every extreme that they name: `zone_width`: zone widths in columns.
All inputs are finite; a program needn't handle non-finite values.
Results may differ from the reference program's by a relative error of at most 0.0001.
Values sent between devices are 32-bit elements; how exact they have to be, the bound alone decides.
No kernel may reach another device: no remote copies, remote signals or barrier semaphores. Data moves between devices by JAX's collectives and lax.ppermute only.
A program may use at most 128 MiB of HBM per device.

```python
import math
import jax
import jax.numpy as jnp
from jax import lax

NZ = 64
SUB = 6
TERRAIN_MAX = 8
ZONE_MAX = 16
NX = 128
NY = 2048


def place_ends(values, rng, least, largest):
    dims = values.shape
    index_at = [jax.random.randint(jax.random.fold_in(rng, axis), (), 0, dims[axis]) for axis in range(len(dims))]
    values = values.at[tuple(index_at)].set(least)
    longest = dims.index(max(dims))
    index_at[longest] = (index_at[longest] + 1) % dims[longest]
    return values.at[tuple(index_at)].set(largest)


def block_scale(key, shape, split, smallest, high):
    gain = 1.0
    for dim, shards_of in split:
        heights = jax.random.uniform(jax.random.fold_in(jax.random.fold_in(key, 6), dim), (shards_of,), jnp.float32, smallest / len(split), high / len(split))
        gain = gain * jnp.repeat(jnp.exp(heights), shape[dim] // shards_of).reshape((-1,) + (1,) * (len(shape) - 1 - dim))
    return gain


def centred(rng, shape, spread, most, split=(), held_as=jnp.bfloat16):
    drawn = jax.random.normal(rng, shape, jnp.float32) * spread
    if len(split) > 0:
        drawn = block_scale(rng, shape, split, -0.22, 0.18) * drawn
    return jnp.clip(drawn, min=-most, max=most).astype(held_as)


def setup_inputs(seed: int = 0) -> dict:
    seeds = jax.random.split(jax.random.key(seed), 9)
    u_wind = centred(seeds[0], (NZ, NX, NY), 1.0, 6.0, ((1, 8), (2, 16)), jnp.float32)
    v_wind = centred(seeds[1], (NZ, NX, NY), 1.0, 6.0, ((1, 8), (2, 16)), jnp.float32)
    w_wind = centred(seeds[2], (NZ, NX, NY), 0.5, 4.0, ((1, 8), (2, 16)), jnp.float32)
    pressure = centred(seeds[3], (NZ, NX, NY), 1.0, 6.0, ((1, 8), (2, 16)), jnp.float32)
    terrain_level = place_ends(jax.random.randint(seeds[4], (NX, NY), 0, TERRAIN_MAX + 1), jax.random.fold_in(seeds[4], 1), 0, TERRAIN_MAX).astype(jnp.int32)
    zone_width = place_ends(jax.random.randint(seeds[5], (4,), ZONE_MAX // 4 + 1, ZONE_MAX + 1), jax.random.fold_in(seeds[5], 1), ZONE_MAX // 4 + 1, ZONE_MAX).astype(jnp.int32)
    stiffness = jnp.clip(jnp.exp(jax.random.uniform(seeds[6], (NZ,), jnp.float32, math.log(0.25), math.log(2.0))), 0.25, 2.0)
    inflow_profile = centred(seeds[7], (2, NZ), 1.0, 5.0, (), jnp.float32)
    return dict(u_wind=u_wind, v_wind=v_wind, w_wind=w_wind, pressure=pressure, terrain_level=terrain_level, zone_width=zone_width, stiffness=stiffness, inflow_profile=inflow_profile)


ADV_COURANT = 0.3
H_COURANT = 0.4
Z_COURANT = 1.0
RELAX_STRENGTH = 0.5


def face_flux(scalar, velocity, along):
    extent = scalar.shape[along]
    count = extent - 5

    def offset(start):
        return lax.slice_in_dim(scalar, start, start + count, axis=along)

    centered = (37.0 * (offset(3) + offset(2)) - 8.0 * (offset(4) + offset(1)) + (offset(5) + offset(0))) / 60.0
    upwind = (10.0 * (offset(3) - offset(2)) - 5.0 * (offset(4) - offset(1)) + (offset(5) - offset(0))) / 60.0
    face_speed = lax.slice_in_dim(velocity, 3, 3 + count, axis=along)
    flux = face_speed * centered - jnp.abs(face_speed) * upwind
    return lax.slice_in_dim(flux, 1, count, axis=along) - lax.slice_in_dim(flux, 0, count - 1, axis=along)


def advect(extended, wet_inner):
    west_east = extended[0]
    south_north = extended[1]
    first = west_east.shape[1]
    second = west_east.shape[2]
    results = []
    for scalar in extended:
        tend_x = face_flux(scalar, west_east, 1)[:, :, 3:second - 3]
        tend_y = face_flux(scalar, south_north, 2)[:, 3:first - 3, :]
        inner = scalar[:, 3:first - 3, 3:second - 3]
        results.append(wet_inner * (inner - ADV_COURANT * (tend_x + tend_y)))
    return results


def relax_plane(col_index, row_index, x_total, y_total, zones):
    zone_f = zones.astype(jnp.float32)
    west_ramp = jnp.maximum(zone_f[0] - col_index, 0.0) / zone_f[0]
    east_ramp = jnp.maximum(zone_f[1] - (x_total - 1.0 - col_index), 0.0) / zone_f[1]
    south_ramp = jnp.maximum(zone_f[2] - row_index, 0.0) / zone_f[2]
    north_ramp = jnp.maximum(zone_f[3] - (y_total - 1.0 - row_index), 0.0) / zone_f[3]
    along_x = jnp.maximum(west_ramp, east_ramp)[:, None]
    along_y = jnp.maximum(south_ramp, north_ramp)[None, :]
    return RELAX_STRENGTH * jnp.maximum(along_x, along_y)


def thomas(sub_diag, main_diag, super_diag, right_side):
    def eliminate(carry, row):
        c_prev, d_prev = carry
        low_row, main_row, up_row, rhs_row = row
        pivot_value = main_row - low_row * c_prev
        c_new = up_row / pivot_value
        d_new = (rhs_row - low_row * d_prev) / pivot_value
        return (c_new, d_new), (c_new, d_new)

    zero_plane = jnp.zeros_like(main_diag[0])
    unused, (c_all, d_all) = lax.scan(eliminate, (zero_plane, zero_plane), (sub_diag, main_diag, super_diag, right_side), unroll=8)

    def substitute(x_next, row):
        c_row, d_row = row
        value = d_row - c_row * x_next
        return value, value

    unused_last, solved = lax.scan(substitute, zero_plane, (c_all, d_all), reverse=True, unroll=8)
    return solved


def shift_down(field):
    return jnp.concatenate([jnp.zeros_like(field[:1]), field[:-1]], axis=0)


def shift_up(field):
    return jnp.concatenate([field[1:], jnp.zeros_like(field[:1])], axis=0)


def column_solve(w_wind, q_field, wet_mask, g_level):
    factor = Z_COURANT * Z_COURANT
    g_cell = g_level * wet_mask
    g_above = shift_up(g_cell)
    wet_below = shift_down(wet_mask)
    sub_diag = -factor * g_cell * wet_below
    super_diag = -factor * g_above * wet_mask
    main_diag = 1.0 + wet_mask * factor * (g_above + g_cell)
    right_side = wet_mask * (w_wind - Z_COURANT * (shift_up(q_field) - q_field))
    return thomas(sub_diag, main_diag, super_diag, right_side)


def local_west(field):
    return jnp.concatenate([jnp.zeros_like(field[:, :1, :]), field[:, :-1, :]], axis=1)


def local_east(field):
    return jnp.concatenate([field[:, 1:, :], jnp.zeros_like(field[:, :1, :])], axis=1)


def local_south(field):
    return jnp.concatenate([jnp.zeros_like(field[:, :, :1]), field[:, :, :-1]], axis=2)


def local_north(field):
    return jnp.concatenate([field[:, :, 1:], jnp.zeros_like(field[:, :, :1])], axis=2)


def substep_update(carried, wet_mask, relax, g_level, u_bound, v_bound, from_west, from_south, from_east, from_north):
    u_wind, v_wind, w_wind, pressure = carried
    u_wind = wet_mask * (u_wind - H_COURANT * (pressure - from_west(pressure)))
    v_wind = wet_mask * (v_wind - H_COURANT * (pressure - from_south(pressure)))
    divergence = H_COURANT * (from_east(u_wind) - u_wind + from_north(v_wind) - v_wind)
    q_field = wet_mask * (pressure - g_level * divergence)
    w_wind = column_solve(w_wind, q_field, wet_mask, g_level)
    pressure = wet_mask * (q_field - g_level * Z_COURANT * (w_wind - shift_down(w_wind)))
    u_wind = u_wind - relax * (u_wind - wet_mask * u_bound)
    v_wind = v_wind - relax * (v_wind - wet_mask * v_bound)
    w_wind = w_wind - relax * w_wind
    pressure = pressure - relax * pressure
    return (u_wind, v_wind, w_wind, pressure)


def reference(u_wind, v_wind, w_wind, pressure, terrain_level, zone_width, stiffness, inflow_profile):
    levels = jnp.arange(NZ).astype(jnp.float32)[:, None, None]
    wet_mask = (levels >= terrain_level.astype(jnp.float32)[None, :, :]).astype(jnp.float32)
    padding = ((0, 0), (3, 3), (3, 3))
    extended = [jnp.pad(field, padding) for field in (u_wind, v_wind, w_wind, pressure)]
    carried = tuple(advect(extended, wet_mask))
    col_index = jnp.arange(NX).astype(jnp.float32)
    row_index = jnp.arange(NY).astype(jnp.float32)
    relax = relax_plane(col_index, row_index, float(NX), float(NY), zone_width)
    g_level = stiffness[:, None, None]
    u_bound = inflow_profile[0][:, None, None]
    v_bound = inflow_profile[1][:, None, None]
    for substep in range(SUB):
        carried = substep_update(carried, wet_mask, relax, g_level, u_bound, v_bound, local_west, local_south, local_east, local_north)
    return carried[0], carried[1], carried[2], carried[3]
```

```python
import jax
import jax.numpy as jnp
from jax import lax
from jax.experimental import pallas as pl
from jax.experimental.pallas import tpu as pltpu
from jax.sharding import PartitionSpec as P

SUB = 6
ADV = 0.3
H = 0.4
RELAX = 0.5
WET_FROM = 8
HALO = 8

f32 = jnp.float32


def vmem():
    return pl.BlockSpec(memory_space=pltpu.VMEM)


def smem():
    return pl.BlockSpec(memory_space=pltpu.SMEM)


def lanes(shape):
    return lax.broadcasted_iota(jnp.int32, shape, len(shape) - 1)


def pack_y_kernel(u, v, w, p, terrain, stiff, inflow, ylo, yhi, coef):
    nz = u.shape[0]
    groups = nz // 8
    lane = lanes((16, 128))
    for f, ref in enumerate((u, v, w, p)):

        def body(g, carry, f=f, ref=ref):
            low = jnp.zeros((16, 128), f32)
            high = jnp.zeros((16, 128), f32)
            for s in range(8):
                value = ref[g * 8 + s]
                here = (lane >= 16 * s) & (lane < 16 * s + 16)
                low = jnp.where(here, pltpu.roll(value, 16 * s, 1), low)
                high = jnp.where(here, pltpu.roll(value, (16 * s - 112) % 128, 1), high)
            ylo[f * groups + g] = low
            yhi[f * groups + g] = high
            return carry

        lax.fori_loop(0, groups, body, 0)
    solid = terrain[...].astype(f32)
    ylo[4 * groups] = solid
    yhi[4 * groups] = solid
    one = jnp.ones((8, 128), f32)
    above = jnp.zeros((8, 128), f32)
    ratio = jnp.zeros((8, 128), f32)
    for k in range(nz - 1, -1, -1):
        g = jnp.full((8, 128), stiff[k], f32)
        inverse = one / (one + g + above * (one - ratio))
        coef[0, k] = inverse
        coef[1, k] = above * inverse
        coef[2, k] = g * inverse
        coef[3, k] = g
        coef[4, k] = (H * H) * g
        coef[5, k] = jnp.full((8, 128), inflow[0, k], f32)
        coef[6, k] = jnp.full((8, 128), inflow[1, k], f32)
        ratio = g * inverse
        above = g


def pack_x_kernel(u, v, w, p, terrain, north, south, uw, ue, vw, ve, ww, we, pw, pe):
    nz = u.shape[0]
    groups = nz // 8
    lane = lanes((16, 128))
    for f, (ref, west, east) in enumerate(((u, uw, ue), (v, vw, ve), (w, ww, we), (p, pw, pe))):
        ninth = f in (0, 3)

        def body(g, carry, f=f, ref=ref, west=west, east=east, ninth=ninth):
            for s in range(8):
                k = g * 8 + s
                west[k] = ref[k, 0:8, :]
                east[k] = ref[k, 8:16, :]
                if ninth:
                    west[nz + groups + g, s : s + 1, :] = ref[k, 8:9, :]
                    east[nz + groups + g, s : s + 1, :] = ref[k, 7:8, :]
            corner = jnp.where(
                lane % 16 < 8,
                pltpu.roll(south[f * groups + g], 120, 1),
                pltpu.roll(north[f * groups + g], 8, 1),
            )
            west[nz + g] = corner[0:8]
            east[nz + g] = corner[8:16]
            return carry

        lax.fori_loop(0, groups, body, 0)
    solid = terrain[...].astype(f32)
    side = side_tile(lane, north[4 * groups], south[4 * groups])
    last = nz + 2 * groups
    uw[last] = solid[0:8]
    ue[last] = solid[8:16]
    uw[last + 1] = side[0:8]
    ue[last + 1] = side[8:16]


def side_tile(lane, north, south):
    return jnp.where(lane < 16, north, jnp.where(lane >= 112, south, 0.0))


def extend(ref, f, north, south, west, east, g, s, ninth):
    nz = ref.shape[0]
    groups = nz // 8
    k = g * 8 + s
    lane16 = lanes((16, 128))
    lane8 = lanes((8, 128))
    own = side_tile(
        lane16,
        pltpu.roll(north[f * groups + g], (-16 * s) % 128, 1),
        pltpu.roll(south[f * groups + g], (112 - 16 * s) % 128, 1),
    )
    edge = (lane8 < 8) | (lane8 >= 120)
    back = (120 - 16 * s) % 128
    corner_west = jnp.where(edge, pltpu.roll(west[nz + g], back, 1), 0.0)
    corner_east = jnp.where(edge, pltpu.roll(east[nz + g], back, 1), 0.0)
    zero = jnp.zeros((8, 128), f32)
    extra = zero
    if ninth:
        row = lax.broadcasted_iota(jnp.int32, (8, 128), 0)
        far_east = jnp.broadcast_to(east[nz + groups + g, s : s + 1, :], (8, 128))
        far_west = jnp.broadcast_to(west[nz + groups + g, s : s + 1, :], (8, 128))
        extra = jnp.where(row == 0, far_east, jnp.where(row == 7, far_west, 0.0))
    main = jnp.concatenate([west[k], ref[k], east[k], extra], axis=0)
    side = jnp.concatenate([corner_west, own, corner_east, zero], axis=0)
    return jnp.concatenate([main, side], axis=1)


def face_difference(value, speed, dim):
    size = value.shape[dim]

    def at(by):
        return pltpu.roll(value, (-by) % size, dim)

    before, after = at(-1), at(1)
    before2, after2 = at(-2), at(2)
    before3 = at(-3)
    centred = 37.0 * (value + before) - 8.0 * (after + before2) + (after2 + before3)
    upwind = 10.0 * (value - before) - 5.0 * (after - before2) + (after2 - before3)
    flux = speed * centred - jnp.abs(speed) * upwind
    return pltpu.roll(flux, size - 1, dim) - flux


def advected(value, u, v):
    scale = ADV / 60.0
    across = face_difference(value, scale * u, 0)[0:32]
    along = face_difference(value[0:32], scale * v[0:32], 1)
    return value[0:32] - (across + along)


def advect_uv_kernel(
    u, v, terrain, zones, north, south, uw, ue, vw, ve, xu, xv, au, av, masks, damp
):
    nz = u.shape[0]
    groups = nz // 8
    lane = lanes((16, 128))
    own_side = side_tile(lane, north[4 * groups], south[4 * groups])
    last = nz + 2 * groups
    solid = jnp.concatenate(
        [
            jnp.concatenate([uw[last], terrain[...].astype(f32), ue[last]], axis=0),
            jnp.concatenate([uw[last + 1], own_side, ue[last + 1]], axis=0),
        ],
        axis=1,
    )
    shape = (32, 256)
    block_x, block_y = u.shape[1], u.shape[2]
    total_x = block_x * lax.axis_size("gx")
    total_y = block_y * lax.axis_size("gy")
    row = lax.broadcasted_iota(jnp.int32, shape, 0) - HALO
    col = lanes(shape)
    col = jnp.where(col < 192, col, col - 256)
    at_x = lax.axis_index("gx") * block_x + row
    at_y = lax.axis_index("gy") * block_y + col
    inside = (at_x >= 0) & (at_x < total_x) & (at_y >= 0) & (at_y < total_y)
    inside = inside & (col < block_y + 16) & (col >= -16)
    inside = jnp.where(inside, 1.0, 0.0).astype(f32)
    for k in range(WET_FROM):
        masks[k] = jnp.where(solid <= float(k), inside, 0.0)
    masks[WET_FROM] = inside
    at_x = at_x.astype(f32)
    at_y = at_y.astype(f32)
    ramp = jnp.zeros(shape, f32)
    for b, distance in enumerate((at_x, (total_x - 1.0) - at_x, at_y, (total_y - 1.0) - at_y)):
        width = jnp.full(shape, zones[b], jnp.int32).astype(f32)
        ramp = jnp.maximum(ramp, jnp.maximum(width - distance, 0.0) / width)
    relax = RELAX * ramp
    damp[0] = jnp.where(inside > 0.0, 1.0 - relax, 0.0)
    damp[1] = jnp.where(inside > 0.0, relax, 0.0)

    def fill(g, carry):
        for s in range(8):
            k = g * 8 + s
            xu[k] = extend(u, 0, north, south, uw, ue, g, s, True)
            xv[k] = extend(v, 1, north, south, vw, ve, g, s, False)
        return carry

    lax.fori_loop(0, groups, fill, 0)

    def level(k, carry):
        mask = masks[jnp.minimum(k, WET_FROM)]
        au[k] = mask * advected(xu[k], xu[k], xv[k])
        av[k] = mask * advected(xv[k], xu[k], xv[k])
        return carry

    lax.fori_loop(0, nz, level, 0)


def advect_one_kernel(x, xu, xv, masks, north, south, west, east, out, *, f):
    nz = x.shape[0]
    groups = nz // 8

    def body(g, carry):
        for s in range(8):
            k = g * 8 + s
            mask = H * masks[jnp.minimum(k, WET_FROM)]
            value = extend(x, f, north, south, west, east, g, s, f == 3)
            out[k] = mask * advected(value, xu[k], xv[k])
        return carry

    lax.fori_loop(0, groups, body, 0)


def splat(tile):
    tall = jnp.concatenate([tile] * 4, axis=0)
    return jnp.concatenate([tall, tall], axis=1)


def substeps_kernel(
    au, av, aw, ap, masks, damp, coef, uo, vo, wo, po, us, vs, ws, ps, qs, ds
):
    nz = au.shape[0]
    zero = jnp.zeros((32, 256), f32)

    for step in range(SUB):
        first, final = step == 0, step == SUB - 1
        ur, vr, wr, pr = (au, av, aw, ap) if first else (us, vs, ws, ps)

        def down(k, carry, masked):
            q_above, d_above = carry
            p = pr[k]
            mask = masks[k] if masked else masks[WET_FROM]
            u = mask * (ur[k] - (p - pltpu.roll(p, 1, 0)))
            v = mask * (vr[k] - (p - pltpu.roll(p, 1, 1)))
            divergence = (pltpu.roll(u, 31, 0) - u) + (pltpu.roll(v, 255, 1) - v)
            q = p - splat(coef[4, k]) * divergence
            d = (wr[k] - (q_above - q)) * splat(coef[0, k]) + splat(coef[1, k]) * d_above
            keep, pull = damp[0], damp[1]
            if masked:
                d = mask * d
                pull = mask * pull
            u = keep * u + pull * splat(coef[5, k])
            v = keep * v + pull * splat(coef[6, k])
            if final:
                uo[k] = u[8:24, 0:128]
                vo[k] = v[8:24, 0:128]
            else:
                us[k] = u
                vs[k] = v
            qs[k] = q
            ds[k] = d
            return q, d

        carry = lax.fori_loop(
            0, nz - WET_FROM, lambda t, c: down(nz - 1 - t, c, False), (zero, zero)
        )
        lax.fori_loop(0, WET_FROM, lambda t, c: down(WET_FROM - 1 - t, c, True), carry)

        def up(k, below, masked):
            w = ds[k] + splat(coef[2, k]) * below
            p = qs[k] - splat(coef[3, k]) * (w - below)
            keep = damp[0]
            if masked:
                p = masks[k] * p
            if final:
                wo[k] = ((1.0 / H) * (keep * w))[8:24, 0:128]
                po[k] = ((1.0 / H) * (keep * p))[8:24, 0:128]
            else:
                ws[k] = keep * w
                ps[k] = keep * p
            return w

        below = lax.fori_loop(0, WET_FROM, lambda k, c: up(k, c, True), zero)
        lax.fori_loop(WET_FROM, nz, lambda k, c: up(k, c, False), below)


def neighbours(axis, by):
    size = lax.axis_size(axis)
    return [(i, i + by) for i in range(size) if 0 <= i + by < size]


def on_device(u, v, w, p, terrain, zones, stiff, inflow):
    nz = u.shape[0]
    groups = nz // 8
    big = pltpu.CompilerParams(vmem_limit_bytes=60 * 1024 * 1024)

    def arr(*shape):
        return jax.ShapeDtypeStruct(shape, f32)

    ylo, yhi, coef = pl.pallas_call(
        pack_y_kernel,
        out_shape=(arr(4 * groups + 1, 16, 128), arr(4 * groups + 1, 16, 128), arr(7, nz, 8, 128)),
        in_specs=[vmem()] * 5 + [smem()] * 2,
        out_specs=(vmem(),) * 3,
        compiler_params=big,
        name="pack_y",
    )(u, v, w, p, terrain, stiff, inflow)
    north = lax.ppermute(ylo, "gy", neighbours("gy", -1))
    south = lax.ppermute(yhi, "gy", neighbours("gy", 1))
    tiles_of = (nz + 2 * groups + 2, nz + groups, nz + groups, nz + 2 * groups)
    sent = pl.pallas_call(
        pack_x_kernel,
        out_shape=tuple(arr(t, 8, 128) for t in tiles_of for _ in range(2)),
        in_specs=[vmem()] * 7,
        out_specs=(vmem(),) * 8,
        compiler_params=big,
        name="pack_x",
    )(u, v, w, p, terrain, north, south)
    east = [lax.ppermute(m, "gx", neighbours("gx", -1)) for m in sent[0::2]]
    west = [lax.ppermute(m, "gx", neighbours("gx", 1)) for m in sent[1::2]]
    xu, xv, au, av, masks, damp = pl.pallas_call(
        advect_uv_kernel,
        out_shape=(
            arr(nz, 40, 256),
            arr(nz, 40, 256),
            arr(nz, 32, 256),
            arr(nz, 32, 256),
            arr(WET_FROM + 1, 32, 256),
            arr(2, 32, 256),
        ),
        in_specs=[vmem()] * 3 + [smem()] + [vmem()] * 6,
        out_specs=(vmem(),) * 6,
        compiler_params=big,
        name="advect_uv",
    )(u, v, terrain, zones, north, south, west[0], east[0], west[1], east[1])

    def advect_one(x, f):
        def kernel(*refs):
            advect_one_kernel(*refs, f=f)

        return pl.pallas_call(
            kernel,
            out_shape=arr(nz, 32, 256),
            in_specs=[vmem()] * 8,
            out_specs=vmem(),
            compiler_params=big,
            name="advect_w" if f == 2 else "advect_p",
        )(x, xu, xv, masks, north, south, west[f], east[f])

    aw = advect_one(w, 2)
    ap = advect_one(p, 3)
    out = arr(nz, 16, 128)
    return pl.pallas_call(
        substeps_kernel,
        out_shape=(out,) * 4,
        in_specs=[vmem()] * 7,
        out_specs=(vmem(),) * 4,
        scratch_shapes=[pltpu.VMEM((nz, 32, 256), f32)] * 6,
        compiler_params=big,
        name="substeps",
    )(au, av, aw, ap, masks, damp, coef)


def solution(mesh):
    field = P(None, "gx", "gy")
    return jax.shard_map(
        on_device,
        mesh=mesh,
        in_specs=(field, field, field, field, P("gx", "gy"), P(), P(), P()),
        out_specs=(field, field, field, field),
        check_vma=False,
    )
```

```python
import jax
import jax.numpy as jnp
import numpy as np
from jax import lax
from jax.experimental import pallas as pl
from jax.experimental.pallas import tpu as pltpu
from jax.sharding import PartitionSpec as P

SUB = 6
ADV = 0.3
H = 0.4
RELAX = 0.5
WET_FROM = 8
HALO = 8

f32 = jnp.float32
UD, UU = 8, 8


def vmem():
    return pl.BlockSpec(memory_space=pltpu.VMEM)


def smem():
    return pl.BlockSpec(memory_space=pltpu.SMEM)


def lanes(shape):
    return lax.broadcasted_iota(jnp.int32, shape, len(shape) - 1)


def pack_a_kernel(u, v, w, p, terrain, ylo, yhi, west, east):
    nz = u.shape[0]
    groups = nz // 8
    lane = lanes((16, 128))
    for f, ref in enumerate((u, v, w, p)):

        def body(g, carry, f=f, ref=ref):
            rolled = []
            for s in range(8):
                k = g * 8 + s
                value = ref[k]
                rolled.append(pltpu.roll(value, 16 * s, 1))
                if f < 2:
                    west[f * nz + k] = value[0:8]
                    east[f * nz + k] = value[8:16]
            low = rolled[0]
            high = rolled[0]
            for s in range(1, 8):
                low = jnp.where(lane // 16 == s, rolled[s], low)
                high = jnp.where(lane // 16 == s - 1, rolled[s], high)
            ylo[f * groups + g] = low
            yhi[f * groups + g] = high
            return carry

        lax.fori_loop(0, groups, body, 0, unroll=2)
    solid = terrain[...].astype(f32)
    ylo[4 * groups] = solid
    yhi[4 * groups] = solid


def pack_b_kernel(w, p, stiff, inflow, north, ww, we, pw, pe, coef):
    nz = w.shape[0]
    for ref, west, east in ((w, ww, we), (p, pw, pe)):
        west[...] = ref[:, 0:8, :]
        east[...] = ref[:, 8:16, :]
    one = jnp.ones((8, 128), f32)
    above = jnp.zeros((8, 128), f32)
    ratio = jnp.zeros((8, 128), f32)
    for k in range(nz - 1, -1, -1):
        g = jnp.full((8, 128), stiff[k], f32)
        inverse = one / (one + g + above * (one - ratio))
        coef[0, k] = inverse
        coef[1, k] = above * inverse
        coef[2, k] = g * inverse
        coef[3, k] = g
        coef[4, k] = (H * H) * g
        coef[5, k] = jnp.full((8, 128), inflow[0, k], f32)
        coef[6, k] = jnp.full((8, 128), inflow[1, k], f32)
        ratio = g * inverse
        above = g


def pack_c_kernel(u, p, terrain, north, south, cw, ce):
    nz = u.shape[0]
    groups = nz // 8
    lane = lanes((16, 128))
    for t in range(4 * groups):
        corner = jnp.where(lane % 16 < 8, north[t], south[t])
        cw[t] = corner[0:8]
        ce[t] = corner[8:16]
    for f, ref in enumerate((u, p)):

        def body(g, carry, f=f, ref=ref):
            for s in range(8):
                cw[(4 + f) * groups + g, s : s + 1, :] = ref[g * 8 + s, 8:9, :]
                ce[(4 + f) * groups + g, s : s + 1, :] = ref[g * 8 + s, 7:8, :]
            return carry

        lax.fori_loop(0, groups, body, 0)
    solid = terrain[...].astype(f32)
    side = side_tile(lane, north[4 * groups], south[4 * groups])
    last = 6 * groups
    cw[last] = solid[0:8]
    ce[last] = solid[8:16]
    cw[last + 1] = side[0:8]
    ce[last + 1] = side[8:16]


def side_tile(lane, north, south):
    return jnp.where(lane < 16, north, jnp.where(lane >= 112, south, 0.0))


def extend(ref, f, north, south, west, east, far_w, far_e, g, s, base=0):
    groups = ref.shape[0] // 8
    k = g * 8 + s
    lane16 = lanes((16, 128))
    lane8 = lanes((8, 128))
    back = (-16 * s) % 128
    t = f * groups + g
    own = side_tile(lane16, pltpu.roll(north[t], back, 1), pltpu.roll(south[t], back, 1))
    edge = (lane8 < 8) | (lane8 >= 120)
    corner_west = jnp.where(edge, pltpu.roll(far_w[t], back, 1), 0.0)
    corner_east = jnp.where(edge, pltpu.roll(far_e[t], back, 1), 0.0)
    zero = jnp.zeros((8, 128), f32)
    extra = zero
    if f in (0, 3):
        t = (4 if f == 0 else 5) * groups + g
        row = lax.broadcasted_iota(jnp.int32, (8, 128), 0)
        ninth_e = jnp.broadcast_to(far_e[t, s : s + 1, :], (8, 128))
        ninth_w = jnp.broadcast_to(far_w[t, s : s + 1, :], (8, 128))
        extra = jnp.where(row == 0, ninth_e, jnp.where(row == 7, ninth_w, 0.0))
    main = jnp.concatenate([west[base + k], ref[k], east[base + k], extra], axis=0)
    side = jnp.concatenate([corner_west, own, corner_east, zero], axis=0)
    return jnp.concatenate([main, side], axis=1)


BAND = ((0, 37, 10), (-1, 37, -10), (1, -8, -5), (-2, -8, 5), (2, 1, 1), (-3, 1, -1))


def band_matrix():
    band = np.zeros((256, 512), np.float32)
    j = np.arange(256)
    for by, centred, upwind in BAND:
        band[(j + by) % 256, j] = centred
        band[(j + by) % 256, 256 + j] = upwind
    return jnp.asarray(band, jnp.bfloat16)


def stage(parts, s, value):
    rows = slice(32 * s, 32 * s + 32)
    for part in parts:
        piece = value.astype(jnp.bfloat16)
        part[rows, :] = piece
        value = value - piece.astype(f32)


def along_sums(parts, band, sums):
    total = jnp.dot(parts[0][...], band[...], preferred_element_type=f32)
    for part in parts[1:]:
        total = total + jnp.dot(part[...], band[...], preferred_element_type=f32)
    sums[...] = total


def advected(value, u, v, sums, s):
    scale = ADV / 60.0

    def at(by):
        return pltpu.roll(value, (-by) % 40, 0)

    before, after = at(-1), at(1)
    before2, after2 = at(-2), at(2)
    before3 = at(-3)
    centred = 37.0 * (value + before) - 8.0 * (after + before2) + (after2 + before3)
    upwind = 10.0 * (value - before) - 5.0 * (after - before2) + (after2 - before3)
    speed = scale * u
    flux = speed * centred - jnp.abs(speed) * upwind
    across = (pltpu.roll(flux, 39, 0) - flux)[0:32]
    rows = slice(32 * s, 32 * s + 32)
    speed = scale * v[0:32]
    flux = speed * sums[rows, 0:256] - jnp.abs(speed) * sums[rows, 256:512]
    along = pltpu.roll(flux, 255, 1) - flux
    return value[0:32] - (across + along)


def advect_uv_kernel(
    u,
    v,
    terrain,
    zones,
    north,
    south,
    cw,
    ce,
    west,
    east,
    band,
    xu,
    xv,
    au,
    av,
    masks,
    damp,
    *scratch,
):
    parts, sums = scratch[0:3], scratch[3]
    nz = u.shape[0]
    groups = nz // 8
    lane = lanes((16, 128))
    own_side = side_tile(lane, north[4 * groups], south[4 * groups])
    last = 6 * groups
    solid = jnp.concatenate(
        [
            jnp.concatenate([cw[last], terrain[...].astype(f32), ce[last]], axis=0),
            jnp.concatenate([cw[last + 1], own_side, ce[last + 1]], axis=0),
        ],
        axis=1,
    )
    shape = (32, 256)
    block_x, block_y = u.shape[1], u.shape[2]
    total_x = block_x * lax.axis_size("gx")
    total_y = block_y * lax.axis_size("gy")
    row = lax.broadcasted_iota(jnp.int32, shape, 0) - HALO
    col = lanes(shape)
    col = jnp.where(col < 192, col, col - 256)
    at_x = lax.axis_index("gx") * block_x + row
    at_y = lax.axis_index("gy") * block_y + col
    inside = (at_x >= 0) & (at_x < total_x) & (at_y >= 0) & (at_y < total_y)
    inside = inside & (col < block_y + 16) & (col >= -16)
    inside = jnp.where(inside, 1.0, 0.0).astype(f32)
    for k in range(WET_FROM):
        masks[k] = jnp.where(solid <= float(k), inside, 0.0)
    masks[WET_FROM] = inside
    at_x = at_x.astype(f32)
    at_y = at_y.astype(f32)
    ramp = jnp.zeros(shape, f32)
    for b, distance in enumerate((at_x, (total_x - 1.0) - at_x, at_y, (total_y - 1.0) - at_y)):
        width = jnp.full(shape, zones[b], jnp.int32).astype(f32)
        ramp = jnp.maximum(ramp, jnp.maximum(width - distance, 0.0) / width)
    relax = RELAX * ramp
    damp[0] = jnp.where(inside > 0.0, 1.0 - relax, 0.0)
    damp[1] = jnp.where(inside > 0.0, relax, 0.0)

    def body(g, carry):
        for s in range(8):
            k = g * 8 + s
            xu[k] = extend(u, 0, north, south, west, east, cw, ce, g, s)
            xv[k] = extend(v, 1, north, south, west, east, cw, ce, g, s, nz)
        for x, out in ((xu, au), (xv, av)):
            for s in range(8):
                stage(parts, s, x[g * 8 + s, 0:32, :])
            along_sums(parts, band, sums)
            for s in range(8):
                k = g * 8 + s
                mask = masks[jnp.minimum(k, WET_FROM)]
                out[k] = mask * advected(x[k], xu[k], xv[k], sums, s)
        return carry

    lax.fori_loop(0, groups, body, 0)


def advect_one_kernel(
    x, xu, xv, masks, north, south, cw, ce, west, east, band, out, *scratch, f
):
    parts, sums, values = scratch[0:3], scratch[3], scratch[4]
    nz = x.shape[0]
    groups = nz // 8

    def body(g, carry):
        for s in range(8):
            value = extend(x, f, north, south, west, east, cw, ce, g, s)
            values[s] = value
            stage(parts, s, value[0:32])
        along_sums(parts, band, sums)
        for s in range(8):
            k = g * 8 + s
            mask = H * masks[jnp.minimum(k, WET_FROM)]
            out[k] = mask * advected(values[s], xu[k], xv[k], sums, s)
        return carry

    lax.fori_loop(0, groups, body, 0)


def advect_scratch():
    part = pltpu.VMEM((256, 256), jnp.bfloat16)
    return [part, part, part, pltpu.VMEM((256, 512), f32)]


def splat(tile):
    tall = jnp.concatenate([tile] * 4, axis=0)
    return jnp.concatenate([tall, tall], axis=1)


def substeps_kernel(
    au, av, aw, ap, masks, damp, coef, uo, vo, wo, po, us, vs, ws, ps, qs, ds
):
    nz = au.shape[0]
    zero = jnp.zeros((32, 256), f32)

    for step in range(SUB):
        first, final = step == 0, step == SUB - 1
        ur, vr, wr, pr = (au, av, aw, ap) if first else (us, vs, ws, ps)

        def down(k, carry, masked):
            q_above, d_above = carry
            p = pr[k]
            mask = masks[k] if masked else masks[WET_FROM]
            u = mask * (ur[k] - (p - pltpu.roll(p, 1, 0)))
            v = mask * (vr[k] - (p - pltpu.roll(p, 1, 1)))
            divergence = (pltpu.roll(u, 31, 0) - u) + (pltpu.roll(v, 255, 1) - v)
            q = p - splat(coef[4, k]) * divergence
            d = (wr[k] - (q_above - q)) * splat(coef[0, k]) + splat(coef[1, k]) * d_above
            keep, pull = damp[0], damp[1]
            if masked:
                d = mask * d
                pull = mask * pull
            u = keep * u + pull * splat(coef[5, k])
            v = keep * v + pull * splat(coef[6, k])
            if final:
                uo[k] = u[8:24, 0:128]
                vo[k] = v[8:24, 0:128]
            else:
                us[k] = u
                vs[k] = v
            qs[k] = q
            ds[k] = d
            return q, d

        carry = lax.fori_loop(
            0, nz - WET_FROM, lambda t, c: down(nz - 1 - t, c, False), (zero, zero), unroll=UD
        )
        lax.fori_loop(0, WET_FROM, lambda t, c: down(WET_FROM - 1 - t, c, True), carry, unroll=UD)

        def up(k, below, masked):
            w = ds[k] + splat(coef[2, k]) * below
            p = qs[k] - splat(coef[3, k]) * (w - below)
            keep = damp[0]
            if masked:
                p = masks[k] * p
            if final:
                wo[k] = ((1.0 / H) * (keep * w))[8:24, 0:128]
                po[k] = ((1.0 / H) * (keep * p))[8:24, 0:128]
            else:
                ws[k] = keep * w
                ps[k] = keep * p
            return w

        below = lax.fori_loop(0, WET_FROM, lambda k, c: up(k, c, True), zero, unroll=UU)
        lax.fori_loop(WET_FROM, nz, lambda k, c: up(k, c, False), below, unroll=UU)


def neighbours(axis, by):
    size = lax.axis_size(axis)
    return [(i, i + by) for i in range(size) if 0 <= i + by < size]


def send(value, axis, by):
    return lax.ppermute(value, axis, neighbours(axis, by))


def on_device(u, v, w, p, terrain, zones, stiff, inflow):
    nz = u.shape[0]
    groups = nz // 8

    def room(mib):
        return pltpu.CompilerParams(vmem_limit_bytes=mib * 1024 * 1024)


    def arr(*shape):
        return jax.ShapeDtypeStruct(shape, f32)

    slab = arr(nz, 8, 128)
    ylo, yhi, uw, ue = pl.pallas_call(
        pack_a_kernel,
        out_shape=(arr(4 * groups + 1, 16, 128),) * 2 + (arr(2 * nz, 8, 128),) * 2,
        in_specs=[vmem()] * 5,
        out_specs=(vmem(),) * 4,
        compiler_params=room(6),
        name="pack_a",
    )(u, v, w, p, terrain)
    north = send(ylo, "gy", -1)
    south = send(yhi, "gy", 1)
    ue_in, uw_in = send(uw, "gx", -1), send(ue, "gx", 1)
    cw, ce = pl.pallas_call(
        pack_c_kernel,
        out_shape=(arr(6 * groups + 2, 8, 128),) * 2,
        in_specs=[vmem()] * 5,
        out_specs=(vmem(),) * 2,
        compiler_params=room(4),
        name="pack_c",
    )(u, p, terrain, north, south)
    ce_in, cw_in = send(cw, "gx", -1), send(ce, "gx", 1)
    ww, we, pw, pe, coef = pl.pallas_call(
        pack_b_kernel,
        out_shape=(slab,) * 4 + (arr(7, nz, 8, 128),),
        in_specs=[vmem()] * 2 + [smem()] * 2 + [pl.BlockSpec(memory_space=pl.ANY)],
        out_specs=(vmem(),) * 5,
        compiler_params=room(6),
        name="pack_b",
    )(w, p, stiff, inflow, north)
    we_in, ww_in = send(ww, "gx", -1), send(we, "gx", 1)
    pe_in, pw_in = send(pw, "gx", -1), send(pe, "gx", 1)
    band = band_matrix()
    advect_uv = pl.pallas_call(
        advect_uv_kernel,
        out_shape=(
            arr(nz, 40, 256),
            arr(nz, 40, 256),
            arr(nz, 32, 256),
            arr(nz, 32, 256),
            arr(WET_FROM + 1, 32, 256),
            arr(2, 32, 256),
        ),
        in_specs=[vmem()] * 3 + [smem()] + [vmem()] * 7,
        out_specs=(vmem(),) * 6,
        scratch_shapes=advect_scratch(),
        compiler_params=room(18),
        name="advect_uv",
    )
    xu, xv, au, av, masks, damp = advect_uv(
        u, v, terrain, zones, north, south, cw_in, ce_in, uw_in, ue_in, band
    )

    def advect_one(x, f, west, east):
        def kernel(*refs):
            advect_one_kernel(*refs, f=f)

        return pl.pallas_call(
            kernel,
            out_shape=arr(nz, 32, 256),
            in_specs=[vmem()] * 11,
            out_specs=vmem(),
            scratch_shapes=advect_scratch() + [pltpu.VMEM((8, 40, 256), f32)],
            compiler_params=room(14),
            name="advect_w" if f == 2 else "advect_p",
        )(x, xu, xv, masks, north, south, cw_in, ce_in, west, east, band)

    aw = advect_one(w, 2, ww_in, we_in)
    ap = advect_one(p, 3, pw_in, pe_in)
    out = arr(nz, 16, 128)
    return pl.pallas_call(
        substeps_kernel,
        out_shape=(out,) * 4,
        in_specs=[vmem()] * 7,
        out_specs=(vmem(),) * 4,
        scratch_shapes=[pltpu.VMEM((nz, 32, 256), f32)] * 6,
        compiler_params=room(28),
        name="substeps",
    )(au, av, aw, ap, masks, damp, coef)


def solution(mesh):
    field = P(None, "gx", "gy")
    return jax.shard_map(
        on_device,
        mesh=mesh,
        in_specs=(field, field, field, field, P("gx", "gy"), P(), P(), P()),
        out_specs=(field, field, field, field),
        check_vma=False,
    )
```

```python
import functools

import jax
import jax.numpy as jnp
import numpy as np
from jax import lax
from jax.experimental import pallas as pl
from jax.experimental.pallas import tpu as pltpu
from jax.sharding import PartitionSpec as P

SUB = 6
ADV = 0.3
H = 0.4
RELAX = 0.5
WET_FROM = 8
HALO = 8

f32 = jnp.float32
UF, UD = 8, 8


def vmem():
    return pl.BlockSpec(memory_space=pltpu.VMEM)


def smem():
    return pl.BlockSpec(memory_space=pltpu.SMEM)


def lanes(shape):
    return lax.broadcasted_iota(jnp.int32, shape, len(shape) - 1)


def pack_a_kernel(u, v, w, p, terrain, ylo, yhi, west, east, *scratch):
    held, sems = scratch[0:4], scratch[4]
    nz = u.shape[0]
    groups = nz // 8
    half = nz // 2
    lane = lanes((16, 128))
    fields = (u, v, w, p)

    def copy(f, part):
        levels = pl.ds(part * half, half)
        return pltpu.make_async_copy(fields[f].at[levels], held[f].at[levels], sems.at[f, part])

    for f in range(4):
        for part in range(2):
            copy(f, part).start()
    solid = terrain[...].astype(f32)
    ylo[4 * groups] = solid
    yhi[4 * groups] = solid
    for f in range(4):
        for part in range(2):
            copy(f, part).wait()

            def body(t, carry, f=f, part=part):
                g = t + part * (groups // 2)
                rolled = []
                for s in range(8):
                    value = held[f][g * 8 + s]
                    rolled.append(pltpu.roll(value, 16 * s, 1))
                    if f < 2:
                        west[f * nz + g * 8 + s] = value[0:8]
                        east[f * nz + g * 8 + s] = value[8:16]
                low = rolled[0]
                high = rolled[0]
                for s in range(1, 8):
                    low = jnp.where(lane // 16 == s, rolled[s], low)
                    high = jnp.where(lane // 16 == s - 1, rolled[s], high)
                ylo[f * groups + g] = low
                yhi[f * groups + g] = high
                return carry

            lax.fori_loop(0, groups // 2, body, 0, unroll=2)


def pack_b_kernel(x, west, east):
    west[...] = x[:, 0:8, :]
    east[...] = x[:, 8:16, :]


def prepare_kernel(stiff, inflow, zones, coef, domain, *, block, nz):
    one = jnp.ones((8, 128), f32)
    above = jnp.zeros((8, 128), f32)
    ratio = jnp.zeros((8, 128), f32)
    for k in range(nz - 1, -1, -1):
        g = jnp.full((8, 128), stiff[k], f32)
        inverse = one / (one + g + above * (one - ratio))
        coef[0, k] = inverse
        coef[1, k] = above * inverse
        coef[2, k] = g * inverse
        coef[3, k] = g
        coef[4, k] = (H * H) * g
        coef[5, k] = jnp.full((8, 128), inflow[0, k], f32)
        coef[6, k] = jnp.full((8, 128), inflow[1, k], f32)
        ratio = g * inverse
        above = g
    shape = (32, 256)
    block_x, block_y = block
    total_x = block_x * lax.axis_size("gx")
    total_y = block_y * lax.axis_size("gy")
    row = lax.broadcasted_iota(jnp.int32, shape, 0) - HALO
    col = lanes(shape)
    col = jnp.where(col < 192, col, col - 256)
    at_x = lax.axis_index("gx") * block_x + row
    at_y = lax.axis_index("gy") * block_y + col
    inside = (at_x >= 0) & (at_x < total_x) & (at_y >= 0) & (at_y < total_y)
    inside = inside & (col < block_y + 16) & (col >= -16)
    inside = jnp.where(inside, 1.0, 0.0).astype(f32)
    at_x = at_x.astype(f32)
    at_y = at_y.astype(f32)
    ramp = jnp.zeros(shape, f32)
    for b, distance in enumerate((at_x, (total_x - 1.0) - at_x, at_y, (total_y - 1.0) - at_y)):
        width = jnp.full(shape, zones[b], jnp.int32).astype(f32)
        ramp = jnp.maximum(ramp, jnp.maximum(width - distance, 0.0) / width)
    relax = RELAX * ramp
    put(domain, 0, inside)
    put(domain, 1, jnp.where(inside > 0.0, 1.0 - relax, 0.0))
    put(domain, 2, jnp.where(inside > 0.0, relax, 0.0))


def put(ref, k, value, start=0):
    rows = slice(start, start + value.shape[0])
    ref[k, 0, rows, :] = value[:, 0:128]
    ref[k, 1, rows, :] = value[:, 128:256]


def both(ref, k, start=0, rows=32):
    at = slice(start, start + rows)
    return jnp.concatenate([ref[k, 0, at, :], ref[k, 1, at, :]], axis=1)


def pack_c_kernel(u, p, terrain, north, south, cw, ce):
    nz = u.shape[0]
    groups = nz // 8
    lane = lanes((16, 128))
    for t in range(4 * groups):
        corner = jnp.where(lane % 16 < 8, north[t], south[t])
        cw[t] = corner[0:8]
        ce[t] = corner[8:16]
    for f, ref in enumerate((u, p)):

        def body(g, carry, f=f, ref=ref):
            for s in range(8):
                cw[(4 + f) * groups + g, s : s + 1, :] = ref[g * 8 + s, 8:9, :]
                ce[(4 + f) * groups + g, s : s + 1, :] = ref[g * 8 + s, 7:8, :]
            return carry

        lax.fori_loop(0, groups, body, 0)
    solid = terrain[...].astype(f32)
    side = side_tile(lane, north[4 * groups], south[4 * groups])
    last = 6 * groups
    cw[last] = solid[0:8]
    ce[last] = solid[8:16]
    cw[last + 1] = side[0:8]
    ce[last + 1] = side[8:16]


def side_tile(lane, north, south):
    return jnp.where(lane < 16, north, jnp.where(lane >= 112, south, 0.0))


def packed_side(f, g, north, south, far_w, far_e, groups):
    t = f * groups + g
    lane = lanes((16, 128))
    own = jnp.where(lane % 16 < 8, north[t], south[t])
    return jnp.concatenate([far_w[t], own, far_e[t]], axis=0)


def extend(main, slot, ref, f, north, south, west, east, far_w, far_e, g, s, base=0):
    groups = ref.shape[0] // 8
    k = g * 8 + s
    lane16 = lanes((16, 128))
    lane8 = lanes((8, 128))
    back = (-16 * s) % 128
    t = f * groups + g
    own = side_tile(lane16, pltpu.roll(north[t], back, 1), pltpu.roll(south[t], back, 1))
    edge = (lane8 < 8) | (lane8 >= 120)
    corner_west = jnp.where(edge, pltpu.roll(far_w[t], back, 1), 0.0)
    corner_east = jnp.where(edge, pltpu.roll(far_e[t], back, 1), 0.0)
    value = jnp.concatenate([west[base + k], ref[k], east[base + k]], axis=0)
    main[slot, 8:40, :] = value
    if f in (0, 3):
        t = (4 if f == 0 else 5) * groups + g
        main[slot, 7:8, :] = far_w[t, s : s + 1, :]
        main[slot, 40:41, :] = far_e[t, s : s + 1, :]
    side = jnp.concatenate([corner_west, own, corner_east], axis=0)
    return value, side


BAND = ((0, 37, 10), (-1, 37, -10), (1, -8, -5), (-2, -8, 5), (2, 1, 1), (-3, 1, -1))


def band_matrix():
    band = np.zeros((256, 512), np.float32)
    j = np.arange(256)
    for by, centred, upwind in BAND:
        band[(j + by) % 256, j] = centred
        band[(j + by) % 256, 256 + j] = upwind
    return jnp.asarray(band, jnp.bfloat16)


def stage(parts, s, value):
    rows = slice(32 * s, 32 * s + 32)
    for part in parts:
        piece = value.astype(jnp.bfloat16)
        part[rows, :] = piece
        value = value - piece.astype(f32)


def along_sums(parts, band, sums):
    total = jnp.dot(parts[0][...], band[...], preferred_element_type=f32)
    for part in parts[1:]:
        total = total + jnp.dot(part[...], band[...], preferred_element_type=f32)
    sums[...] = total


def across_tendency(ref, slot, speed, flux_ref):
    def at(by):
        return ref[slot, 8 + by : 40 + by, :]

    value, before, after = at(0), at(-1), at(1)
    before2, after2 = at(-2), at(2)
    before3 = at(-3)
    centred = 37.0 * (value + before) - 8.0 * (after + before2) + (after2 + before3)
    upwind = 10.0 * (value - before) - 5.0 * (after - before2) + (after2 - before3)
    flux = speed * centred - jnp.abs(speed) * upwind
    flux_ref[slot, 0:32, :] = flux
    return flux_ref[slot, 1:33, :] - flux


def side_across(f, g, sources, groups, packed, flux_ref):
    speed = (ADV / 60.0) * packed_side(0, g, *sources, groups)
    packed[0, 8:40, :] = packed_side(f, g, *sources, groups)
    return across_tendency(packed, 0, speed, flux_ref)


def less_across(main, slot, side, speed, across, s, flux_ref):
    own = across_tendency(main, slot, (ADV / 60.0) * speed, flux_ref)
    across = jnp.concatenate([own, pltpu.roll(across, (-16 * s) % 128, 1)], axis=1)
    return jnp.concatenate([main[slot, 8:40, :], side], axis=1) - across


def along_tendency(v, sums, s):
    rows = slice(32 * s, 32 * s + 32)
    speed = (ADV / 60.0) * v
    flux = speed * sums[rows, 0:256] - jnp.abs(speed) * sums[rows, 256:512]
    return pltpu.roll(flux, 255, 1) - flux


def advect_uv_kernel(
    u,
    v,
    terrain,
    domain,
    north,
    south,
    cw,
    ce,
    west,
    east,
    band,
    xu,
    xv,
    au,
    av,
    masks,
    *scratch,
):
    parts, sums = (scratch[0:3], scratch[3:6]), scratch[6:8]
    vs, sides, packed, flux = scratch[8:12]
    nz = u.shape[0]
    groups = nz // 8
    lane = lanes((16, 128))
    own_side = side_tile(lane, north[4 * groups], south[4 * groups])
    last = 6 * groups
    solid = jnp.concatenate(
        [
            jnp.concatenate([cw[last], terrain[...].astype(f32), ce[last]], axis=0),
            jnp.concatenate([cw[last + 1], own_side, ce[last + 1]], axis=0),
        ],
        axis=1,
    )
    inside = both(domain, 0)
    for k in range(WET_FROM):
        put(masks, k, jnp.where(solid <= float(k), inside, 0.0))
    put(masks, WET_FROM, inside)

    def body(g, carry):
        sources = north, south, cw, ce
        arrived = (*sources[0:2], west, east, *sources[2:4])
        for s in range(8):
            k = g * 8 + s
            main, side = extend(xu, k, u, 0, *arrived, g, s)
            sides[s] = side
            stage(parts[0], s, jnp.concatenate([main, side], axis=1))
        along_sums(parts[0], band, sums[0])
        for s in range(8):
            main, side = extend(vs, s, v, 1, *arrived, g, s, nz)
            whole = jnp.concatenate([main, side], axis=1)
            put(xv, g * 8 + s, whole)
            stage(parts[1], s, whole)
        along_sums(parts[1], band, sums[1])
        for f in range(2):
            across = side_across(f, g, sources, groups, packed, flux)
            for s in range(8):
                k = g * 8 + s
                main, slot = ((xu, k), (vs, s))[f]
                side = sides[s] if f == 0 else xv[k, 1]
                rest = less_across(main, slot, side, xu[k, 8:40, :], across, s, flux)
                value = rest - along_tendency(both(xv, k), sums[f], s)
                put((au, av)[f], k, both(masks, jnp.minimum(k, WET_FROM)) * value)
        return carry

    lax.fori_loop(0, groups, body, 0)


def advect_one_kernel(
    x, xu, xv, masks, north, south, cw, ce, west, east, band, out, *scratch, f
):
    parts, sums = (scratch[0:3], scratch[3:6]), scratch[6:8]
    mains, sides, packed, flux = scratch[8:12]
    nz = x.shape[0]
    groups = nz // 8
    start = 8 if f == 3 else 0

    def body(t, carry):
        sources = north, south, cw, ce
        arrived = (*sources[0:2], west, east, *sources[2:4])
        for h in range(2):
            for s in range(8):
                main, side = extend(mains, 8 * h + s, x, f, *arrived, 2 * t + h, s)
                sides[8 * h + s] = side
                stage(parts[h], s, jnp.concatenate([main, side], axis=1))
            along_sums(parts[h], band, sums[h])
        for h in range(2):
            g = 2 * t + h
            across = side_across(f, g, sources, groups, packed, flux)
            for s in range(8):
                k, n = g * 8 + s, 8 * h + s
                rest = less_across(mains, n, sides[n], xu[k, 8:40, :], across, s, flux)
                value = rest - along_tendency(both(xv, k), sums[h], s)
                put(out, k, H * both(masks, jnp.minimum(k, WET_FROM)) * value, start)
        return carry

    lax.fori_loop(0, groups // 2, body, 0)


def advect_scratch(levels, fluxes):
    part = pltpu.VMEM((256, 256), jnp.bfloat16)
    shapes = ((levels, 48), (levels, 32), (1, 48), (fluxes, 40))
    held = [pltpu.VMEM((count, rows, 128), f32) for count, rows in shapes]
    return [part] * 6 + [pltpu.VMEM((256, 512), f32)] * 2 + held


def splat(tile, shape):
    tall = jnp.concatenate([tile] * (shape[0] // 8), axis=0)
    return jnp.concatenate([tall] * (shape[1] // 128), axis=1)


def substeps_kernel(
    au, av, aw, ap, masks, domain, coef, uo, vo, wo, po, us, vs, ws, ps, qs, ds
):
    nz = au.shape[0]

    for step in range(SUB):
        first, final = step == 0, step == SUB - 1
        ur, vr, wr, pr = (au, av, aw, ap) if first else (us, vs, ws, ps)

        def relaxed(value, keep, pull):
            return value if first else keep * value + pull

        def faces(k, masked):
            if final:
                keep, pull = domain[1, 0, 8:32, :], domain[2, 0, 8:32, :]
                keep_v, pull_v = both(domain, 1, 8, 16), both(domain, 2, 8, 16)
                if masked:
                    mask = both(masks, k, 8, 24)
                    pull, pull_v = mask[:, 0:128] * pull, mask[0:16] * pull_v
                u = relaxed(ur[k, 0, 8:32, :], keep, pull * splat(coef[5, k], (24, 128)))
                u = u - (pr[k, 0, 16:40, :] - pr[k, 0, 15:39, :])
                v = relaxed(both(vr, k, 8, 16), keep_v, pull_v * splat(coef[6, k], (16, 256)))
                p = both(pr, k, 16, 16)
                v = v - (p - pltpu.roll(p, 1, 1))
                if masked:
                    u, v = mask[:, 0:128] * u, mask[0:16] * v
                else:
                    u = jnp.concatenate([u[0:16], domain[0, 0, 24:32, :] * u[16:24]], axis=0)
                    far = domain[0, 1, 8:24, :] * v[:, 128:256]
                    v = jnp.concatenate([v[:, 0:128], far], axis=1)
                us[k, 0, 8:32, :] = u
                put(vs, k, v, 8)
                return
            keep, pull = both(domain, 1), both(domain, 2)
            p = both(pr, k, 8)
            if masked:
                mask = both(masks, k)
                pull = mask * pull
            u = relaxed(both(ur, k), keep, pull * splat(coef[5, k], p.shape))
            v = relaxed(both(vr, k), keep, pull * splat(coef[6, k], p.shape))
            u = u - (p - both(pr, k, 7))
            v = v - (p - pltpu.roll(p, 1, 1))
            if masked:
                u, v = mask * u, mask * v
            else:
                far = both(domain, 0, 24, 8) * u[24:32]
                u = jnp.concatenate([u[0:24], far], axis=0)
                far = domain[0, 1] * v[:, 128:256]
                v = jnp.concatenate([v[:, 0:128], far], axis=1)
            put(us, k, u)
            put(vs, k, v)

        def down(k, carry, masked):
            q_above, d_above = carry
            if final:
                u, u_east = us[k, 0, 8:24, :], us[k, 0, 9:25, :]
                v_all = both(vs, k, 8, 16)
                v, v_north = v_all[:, 0:128], pltpu.roll(v_all, 255, 1)[:, 0:128]
                p, w = pr[k, 0, 16:32, :], wr[k, 0, 8:24, :]
            else:
                u, u_east = both(us, k), both(us, k, 1)
                v = both(vs, k)
                v_north = pltpu.roll(v, 255, 1)
                p, w = both(pr, k, 8), both(wr, k)

            def level(n):
                return splat(coef[n, k], p.shape)

            divergence = (u_east - u) + (v_north - v)
            q = p - level(4) * divergence
            d = (w - (q_above - q)) * level(0) + level(1) * d_above
            if masked:
                mask = masks[k, 0, 8:24, :] if final else both(masks, k)
                d = mask * d
            if final:
                keep, pull = domain[1, 0, 8:24, :], domain[2, 0, 8:24, :]
                if masked:
                    pull = mask * pull
                uo[k] = keep * u + pull * level(5)
                vo[k] = keep * v + pull * level(6)
                qs[k, 0, 8:24, :] = q
                ds[k, 0, 8:24, :] = d
            else:
                put(qs, k, q)
                put(ds, k, d)
            return q, d

        def each_face(k, carry, masked):
            faces(k, masked)
            return carry

        lax.fori_loop(0, WET_FROM, lambda k, c: each_face(k, c, True), 0, unroll=UF)
        lax.fori_loop(WET_FROM, nz, lambda k, c: each_face(k, c, False), 0, unroll=28)
        zero = jnp.zeros((16, 128) if final else (32, 256), f32)
        carry = lax.fori_loop(
            0, nz - WET_FROM, lambda t, c: down(nz - 1 - t, c, False), (zero, zero), unroll=14
        )
        lax.fori_loop(
            0, WET_FROM, lambda t, c: down(WET_FROM - 1 - t, c, True), carry, unroll=UD
        )

        def up(k, below, masked):
            def level(n):
                return splat(coef[n, k], below.shape)

            if final:
                d, q = ds[k, 0, 8:24, :], qs[k, 0, 8:24, :]
                keep = domain[1, 0, 8:24, :]
            else:
                d, q, keep = both(ds, k), both(qs, k), both(domain, 1)
            w = d + level(2) * below
            p = q - level(3) * (w - below)
            if masked:
                p = (masks[k, 0, 8:24, :] if final else both(masks, k)) * p
            if final:
                wo[k] = (1.0 / H) * (keep * w)
                po[k] = (1.0 / H) * (keep * p)
            else:
                put(ws, k, keep * w)
                put(ps, k, keep * p, 8)
            return w

        below = lax.fori_loop(0, WET_FROM, lambda k, c: up(k, c, True), zero, unroll=8)
        lax.fori_loop(WET_FROM, nz, lambda k, c: up(k, c, False), below, unroll=8)


def neighbours(axis, by):
    size = lax.axis_size(axis)
    return [(i, i + by) for i in range(size) if 0 <= i + by < size]


def send(value, axis, by):
    return lax.ppermute(value, axis, neighbours(axis, by))


def on_device(u, v, w, p, terrain, zones, stiff, inflow):
    nz = u.shape[0]
    groups = nz // 8

    def room(mib):
        return pltpu.CompilerParams(vmem_limit_bytes=mib * 1024 * 1024)


    def arr(*shape):
        return jax.ShapeDtypeStruct(shape, f32)

    hbm = pl.BlockSpec(memory_space=pltpu.HBM)
    in_hbm = [pltpu.with_memory_space_constraint(x, pltpu.HBM) for x in (u, v, w, p)]
    ylo, yhi, uw, ue = pl.pallas_call(
        pack_a_kernel,
        out_shape=(arr(4 * groups + 1, 16, 128),) * 2 + (arr(2 * nz, 8, 128),) * 2,
        in_specs=[hbm] * 4 + [vmem()],
        out_specs=(vmem(),) * 4,
        scratch_shapes=[pltpu.VMEM((nz, 16, 128), f32)] * 4 + [pltpu.SemaphoreType.DMA((4, 2))],
        compiler_params=room(8),
        name="pack_a",
    )(*in_hbm, terrain)
    north = send(ylo, "gy", -1)
    south = send(yhi, "gy", 1)
    ue_in, uw_in = send(uw, "gx", -1), send(ue, "gx", 1)

    def slabs(x):
        return pl.pallas_call(
            pack_b_kernel,
            out_shape=(arr(nz, 8, 128),) * 2,
            in_specs=[vmem()],
            out_specs=(vmem(),) * 2,
            compiler_params=room(4),
        )(x)

    ww, we = slabs(w)
    we_in, ww_in = send(ww, "gx", -1), send(we, "gx", 1)
    pw, pe = slabs(p)
    pe_in, pw_in = send(pw, "gx", -1), send(pe, "gx", 1)
    cw, ce = pl.pallas_call(
        pack_c_kernel,
        out_shape=(arr(6 * groups + 2, 8, 128),) * 2,
        in_specs=[vmem()] * 5,
        out_specs=(vmem(),) * 2,
        compiler_params=room(4),
        name="pack_c",
    )(u, p, terrain, north, south)
    ce_in, cw_in = send(cw, "gx", -1), send(ce, "gx", 1)
    prepare = pl.pallas_call(
        functools.partial(prepare_kernel, block=u.shape[1:], nz=nz),
        out_shape=(arr(7, nz, 8, 128), arr(3, 2, 32, 128)),
        in_specs=[smem()] * 3,
        out_specs=(vmem(),) * 2,
        compiler_params=room(8),
        name="prepare",
    )
    coef, domain = prepare(stiff, inflow, zones)
    band = band_matrix()
    advect_uv = pl.pallas_call(
        advect_uv_kernel,
        out_shape=(arr(nz, 48, 128),)
        + (arr(nz, 2, 32, 128),) * 3
        + (arr(WET_FROM + 1, 2, 32, 128),),
        in_specs=[vmem()] * 11,
        out_specs=(vmem(),) * 5,
        scratch_shapes=advect_scratch(8, 64),
        compiler_params=room(20),
        name="advect_uv",
    )
    xu, xv, au, av, masks = advect_uv(
        u, v, terrain, domain, north, south, cw_in, ce_in, uw_in, ue_in, band
    )

    def advect_one(x, f, west, east):
        def kernel(*refs):
            advect_one_kernel(*refs, f=f)

        return pl.pallas_call(
            kernel,
            out_shape=arr(nz, 2, 40 if f == 3 else 32, 128),
            in_specs=[vmem()] * 11,
            out_specs=vmem(),
            scratch_shapes=advect_scratch(16, 16),
            compiler_params=room(16),
            name="advect_w" if f == 2 else "advect_p",
        )(x, xu, xv, masks, north, south, cw_in, ce_in, west, east, band)

    aw = advect_one(w, 2, ww_in, we_in)
    ap = advect_one(p, 3, pw_in, pe_in)
    out = arr(nz, 16, 128)
    return pl.pallas_call(
        substeps_kernel,
        out_shape=(out,) * 4,
        in_specs=[vmem()] * 7,
        out_specs=(vmem(),) * 4,
        scratch_shapes=[
            pltpu.VMEM((nz, 2, rows, 128), f32) for rows in (40, 32, 32, 40, 32, 32)
        ],
        compiler_params=room(34),
        name="substeps",
    )(au, av, aw, ap, masks, domain, coef)


def solution(mesh):
    field = P(None, "gx", "gy")
    return jax.shard_map(
        on_device,
        mesh=mesh,
        in_specs=(field, field, field, field, P("gx", "gy"), P(), P(), P()),
        out_specs=(field, field, field, field),
        check_vma=False,
    )
```

```python
import functools

import jax
import jax.numpy as jnp
import numpy as np
from jax import lax
from jax.experimental import pallas as pl
from jax.experimental.pallas import tpu as pltpu
from jax.sharding import PartitionSpec as P

SUB = 6
ADV = 0.3
H = 0.4
RELAX = 0.5
WET_FROM = 8
HALO = 8

f32 = jnp.float32
UF, UD = 8, 8


def vmem():
    return pl.BlockSpec(memory_space=pltpu.VMEM)


def smem():
    return pl.BlockSpec(memory_space=pltpu.SMEM)


def lanes(shape):
    return lax.broadcasted_iota(jnp.int32, shape, len(shape) - 1)


def pack_a_kernel(u, v, w, p, terrain, ylo, yhi, west, east, *scratch):
    held, sems = scratch[0:4], scratch[4]
    nz = u.shape[0]
    groups = nz // 8
    half = nz // 2
    lane = lanes((16, 128))
    fields = (u, v, w, p)

    def copy(f, part):
        levels = pl.ds(part * half, half)
        return pltpu.make_async_copy(fields[f].at[levels], held[f].at[levels], sems.at[f, part])

    for f in range(4):
        for part in range(2):
            copy(f, part).start()
    ground = pltpu.make_async_copy(terrain, scratch[5], scratch[6])
    ground.start()
    for f in range(4):
        for part in range(2):
            copy(f, part).wait()

            def body(t, carry, f=f, part=part):
                g = t + part * (groups // 2)
                rolled = []
                for s in range(8):
                    value = held[f][g * 8 + s]
                    rolled.append(pltpu.roll(value, 16 * s, 1))
                    if f < 2:
                        west[f * nz + g * 8 + s] = value[0:8]
                        east[f * nz + g * 8 + s] = value[8:16]
                low = rolled[0]
                high = rolled[0]
                for s in range(1, 8):
                    low = jnp.where(lane // 16 == s, rolled[s], low)
                    high = jnp.where(lane // 16 == s - 1, rolled[s], high)
                ylo[f * groups + g] = low
                yhi[f * groups + g] = high
                return carry

            lax.fori_loop(0, groups // 2, body, 0, unroll=4)
    ground.wait()
    solid = scratch[5][...].astype(f32)
    ylo[4 * groups] = solid
    yhi[4 * groups] = solid


def pack_b_kernel(x, west, east):
    west[...] = x[:, 0:8, :]
    east[...] = x[:, 8:16, :]


def prepare_kernel(stiff, inflow, zones, coef, domain, *, block, nz):
    one = jnp.ones((8, 128), f32)
    above = jnp.zeros((8, 128), f32)
    ratio = jnp.zeros((8, 128), f32)
    for k in range(nz - 1, -1, -1):
        g = jnp.full((8, 128), stiff[k], f32)
        inverse = one / (one + g + above * (one - ratio))
        coef[0, k] = inverse
        coef[1, k] = above * inverse
        coef[2, k] = g * inverse
        coef[3, k] = g
        coef[4, k] = (H * H) * g
        coef[5, k] = jnp.full((8, 128), inflow[0, k], f32)
        coef[6, k] = jnp.full((8, 128), inflow[1, k], f32)
        ratio = g * inverse
        above = g
    shape = (32, 256)
    block_x, block_y = block
    total_x = block_x * lax.axis_size("gx")
    total_y = block_y * lax.axis_size("gy")
    row = lax.broadcasted_iota(jnp.int32, shape, 0) - HALO
    col = lanes(shape)
    col = jnp.where(col < 192, col, col - 256)
    at_x = lax.axis_index("gx") * block_x + row
    at_y = lax.axis_index("gy") * block_y + col
    inside = (at_x >= 0) & (at_x < total_x) & (at_y >= 0) & (at_y < total_y)
    inside = inside & (col < block_y + 16) & (col >= -16)
    inside = jnp.where(inside, 1.0, 0.0).astype(f32)
    at_x = at_x.astype(f32)
    at_y = at_y.astype(f32)
    ramp = jnp.zeros(shape, f32)
    for b, distance in enumerate((at_x, (total_x - 1.0) - at_x, at_y, (total_y - 1.0) - at_y)):
        width = jnp.full(shape, zones[b], jnp.int32).astype(f32)
        ramp = jnp.maximum(ramp, jnp.maximum(width - distance, 0.0) / width)
    relax = RELAX * ramp
    put(domain, 0, inside)
    put(domain, 1, jnp.where(inside > 0.0, 1.0 - relax, 0.0))
    put(domain, 2, jnp.where(inside > 0.0, relax, 0.0))


def put(ref, k, value, start=0):
    rows = slice(start, start + value.shape[0])
    ref[k, 0, rows, :] = value[:, 0:128]
    ref[k, 1, rows, :] = value[:, 128:256]


def both(ref, k, start=0, rows=32):
    at = slice(start, start + rows)
    return jnp.concatenate([ref[k, 0, at, :], ref[k, 1, at, :]], axis=1)


def pack_c_kernel(u, p, terrain, north, south, cw, ce):
    nz = u.shape[0]
    groups = nz // 8
    lane = lanes((16, 128))
    for t in range(4 * groups):
        corner = jnp.where(lane % 16 < 8, north[t], south[t])
        cw[t] = corner[0:8]
        ce[t] = corner[8:16]

    def body(g, carry):
        for s in range(8):
            k, row = g * 8 + s, slice(s, s + 1)
            cw[4 * groups + g, row, :] = p[k, 8:9, :]
            ce[4 * groups + g, row, :] = p[k, 7:8, :]
            cw[5 * groups + 2 + g, row, :] = u[k, 8:9, :]
        return carry

    lax.fori_loop(0, groups, body, 0)
    solid = terrain[...].astype(f32)
    side = side_tile(lane, north[4 * groups], south[4 * groups])
    last = 5 * groups
    cw[last] = solid[0:8]
    ce[last] = solid[8:16]
    cw[last + 1] = side[0:8]
    ce[last + 1] = side[8:16]


def side_tile(lane, north, south):
    return jnp.where(lane < 16, north, jnp.where(lane >= 112, south, 0.0))


def packed_side(f, g, north, south, far_w, far_e, groups):
    t = f * groups + g
    lane = lanes((16, 128))
    own = jnp.where(lane % 16 < 8, north[t], south[t])
    return jnp.concatenate([far_w[t], own, far_e[t]], axis=0)


def extend(main, slot, ref, f, north, south, west, east, far_w, far_e, g, s, base=0):
    groups = ref.shape[0] // 8
    k = g * 8 + s
    lane16 = lanes((16, 128))
    lane8 = lanes((8, 128))
    back = (-16 * s) % 128
    t = f * groups + g
    own = side_tile(lane16, pltpu.roll(north[t], back, 1), pltpu.roll(south[t], back, 1))
    edge = (lane8 < 8) | (lane8 >= 120)
    corner_west = jnp.where(edge, pltpu.roll(far_w[t], back, 1), 0.0)
    corner_east = jnp.where(edge, pltpu.roll(far_e[t], back, 1), 0.0)
    value = jnp.concatenate([west[base + k], ref[k], east[base + k]], axis=0)
    main[slot, 8:40, :] = value
    if f in (0, 3):
        if f == 3:
            main[slot, 7:8, :] = far_w[4 * groups + g, s : s + 1, :]
        t = 4 * groups + g + (groups + 2 if f == 0 else 0)
        main[slot, 40:41, :] = far_e[t, s : s + 1, :]
    side = jnp.concatenate([corner_west, own, corner_east], axis=0)
    return value, side


BAND = ((0, 37, 10), (-1, 37, -10), (1, -8, -5), (-2, -8, 5), (2, 1, 1), (-3, 1, -1))


def band_matrix():
    band = np.zeros((256, 512), np.float32)
    j = np.arange(256)
    for by, centred, upwind in BAND:
        band[(j + by) % 256, j] = centred
        band[(j + by) % 256, 256 + j] = upwind
    return jnp.asarray(band, jnp.bfloat16)


def stage(parts, s, value):
    rows = slice(32 * s, 32 * s + 32)
    for part in parts:
        piece = value.astype(jnp.bfloat16)
        part[rows, :] = piece
        value = value - piece.astype(f32)


def along_sums(parts, band, sums):
    total = jnp.dot(parts[0][...], band[...], preferred_element_type=f32)
    for part in parts[1:]:
        total = total + jnp.dot(part[...], band[...], preferred_element_type=f32)
    sums[...] = total


def across_tendency(ref, slot, speed, flux_ref):
    def at(by):
        return ref[slot, 8 + by : 40 + by, :]

    value, before, after = at(0), at(-1), at(1)
    before2, after2 = at(-2), at(2)
    before3 = at(-3)
    centred = 37.0 * (value + before) - 8.0 * (after + before2) + (after2 + before3)
    upwind = 10.0 * (value - before) - 5.0 * (after - before2) + (after2 - before3)
    flux = speed * centred - jnp.abs(speed) * upwind
    flux_ref[slot, 0:32, :] = flux
    return flux_ref[slot, 1:33, :] - flux


def side_across(f, g, sources, groups, packed, flux_ref):
    speed = (ADV / 60.0) * packed_side(0, g, *sources, groups)
    packed[0, 8:40, :] = packed_side(f, g, *sources, groups)
    return across_tendency(packed, 0, speed, flux_ref)


def less_across(main, slot, side, speed, across, s, flux_ref):
    own = across_tendency(main, slot, (ADV / 60.0) * speed, flux_ref)
    across = jnp.concatenate([own, pltpu.roll(across, (-16 * s) % 128, 1)], axis=1)
    return jnp.concatenate([main[slot, 8:40, :], side], axis=1) - across


def along_tendency(v, sums, s):
    rows = slice(32 * s, 32 * s + 32)
    speed = (ADV / 60.0) * v
    flux = speed * sums[rows, 0:256] - jnp.abs(speed) * sums[rows, 256:512]
    return pltpu.roll(flux, 255, 1) - flux


def advect_uv_kernel(
    u,
    v,
    terrain,
    domain,
    north,
    south,
    cw,
    ce,
    west,
    east,
    band,
    xu,
    xv,
    au,
    av,
    masks,
    *scratch,
):
    parts, sums = (scratch[0:3], scratch[3:6]), scratch[6:8]
    vs, sides, packed, flux = scratch[8:12]
    nz = u.shape[0]
    groups = nz // 8
    lane = lanes((16, 128))
    own_side = side_tile(lane, north[4 * groups], south[4 * groups])
    last = 5 * groups
    solid = jnp.concatenate(
        [
            jnp.concatenate([cw[last], terrain[...].astype(f32), ce[last]], axis=0),
            jnp.concatenate([cw[last + 1], own_side, ce[last + 1]], axis=0),
        ],
        axis=1,
    )
    inside = both(domain, 0)
    for k in range(WET_FROM):
        put(masks, k, jnp.where(solid <= float(k), inside, 0.0))
    put(masks, WET_FROM, inside)

    def body(g, carry):
        sources = north, south, cw, ce
        arrived = (*sources[0:2], west, east, *sources[2:4])
        for s in range(8):
            k = g * 8 + s
            main, side = extend(xu, k, u, 0, *arrived, g, s)
            sides[s] = side
            stage(parts[0], s, jnp.concatenate([main, side], axis=1))
        along_sums(parts[0], band, sums[0])
        for s in range(8):
            main, side = extend(vs, s, v, 1, *arrived, g, s, nz)
            whole = jnp.concatenate([main, side], axis=1)
            put(xv, g * 8 + s, whole)
            stage(parts[1], s, whole)
        along_sums(parts[1], band, sums[1])
        for f in range(2):
            across = side_across(f, g, sources, groups, packed, flux)
            for s in range(8):
                k = g * 8 + s
                main, slot = ((xu, k), (vs, s))[f]
                side = sides[s] if f == 0 else xv[k, 1]
                rest = less_across(main, slot, side, xu[k, 8:40, :], across, s, flux)
                value = rest - along_tendency(both(xv, k), sums[f], s)
                put((au, av)[f], k, both(masks, jnp.minimum(k, WET_FROM)) * value)
        return carry

    lax.fori_loop(0, groups, body, 0)


def advect_one_kernel(
    x, xu, xv, masks, north, south, cw, ce, west, east, band, out, *scratch, f
):
    parts, sums = (scratch[0:3], scratch[3:6]), scratch[6:8]
    mains, sides, packed, flux = scratch[8:12]
    nz = x.shape[0]
    groups = nz // 8
    start = 8 if f == 3 else 0

    def body(t, carry):
        sources = north, south, cw, ce
        arrived = (*sources[0:2], west, east, *sources[2:4])
        for h in range(2):
            for s in range(8):
                main, side = extend(mains, 8 * h + s, x, f, *arrived, 2 * t + h, s)
                sides[8 * h + s] = side
                stage(parts[h], s, jnp.concatenate([main, side], axis=1))
            along_sums(parts[h], band, sums[h])
        for h in range(2):
            g = 2 * t + h
            across = side_across(f, g, sources, groups, packed, flux)
            for s in range(8):
                k, n = g * 8 + s, 8 * h + s
                rest = less_across(mains, n, sides[n], xu[k, 8:40, :], across, s, flux)
                value = rest - along_tendency(both(xv, k), sums[h], s)
                put(out, k, H * both(masks, jnp.minimum(k, WET_FROM)) * value, start)
        return carry

    lax.fori_loop(0, groups // 2, body, 0, unroll=4)


def advect_scratch(levels, fluxes):
    part = pltpu.VMEM((256, 256), jnp.bfloat16)
    shapes = ((levels, 48), (levels, 32), (1, 48), (fluxes, 40))
    held = [pltpu.VMEM((count, rows, 128), f32) for count, rows in shapes]
    return [part] * 6 + [pltpu.VMEM((256, 512), f32)] * 2 + held


def splat(tile, shape):
    tall = jnp.concatenate([tile] * (shape[0] // 8), axis=0)
    return jnp.concatenate([tall] * (shape[1] // 128), axis=1)


def substeps_kernel(
    au, av, aw, ap, masks, domain, coef, uo, vo, wo, po, us, vs, ws, ps, qs, ds
):
    nz = au.shape[0]

    for step in range(SUB):
        first, final = step == 0, step == SUB - 1
        ur, vr, wr, pr = (au, av, aw, ap) if first else (us, vs, ws, ps)

        def relaxed(value, keep, pull):
            return value if first else keep * value + pull

        def faces(k, masked):
            if final:
                keep, pull = domain[1, 0, 8:32, :], domain[2, 0, 8:32, :]
                keep_v, pull_v = both(domain, 1, 8, 16), both(domain, 2, 8, 16)
                if masked:
                    mask = both(masks, k, 8, 24)
                    pull, pull_v = mask[:, 0:128] * pull, mask[0:16] * pull_v
                u = relaxed(ur[k, 0, 8:32, :], keep, pull * splat(coef[5, k], (24, 128)))
                u = u - (pr[k, 0, 16:40, :] - pr[k, 0, 15:39, :])
                v = relaxed(both(vr, k, 8, 16), keep_v, pull_v * splat(coef[6, k], (16, 256)))
                p = both(pr, k, 16, 16)
                v = v - (p - pltpu.roll(p, 1, 1))
                if masked:
                    u, v = mask[:, 0:128] * u, mask[0:16] * v
                else:
                    u = jnp.concatenate([u[0:16], domain[0, 0, 24:32, :] * u[16:24]], axis=0)
                    far = domain[0, 1, 8:24, :] * v[:, 128:256]
                    v = jnp.concatenate([v[:, 0:128], far], axis=1)
                us[k, 0, 8:32, :] = u
                put(vs, k, v, 8)
                return
            keep, pull = both(domain, 1), both(domain, 2)
            p = both(pr, k, 8)
            if masked:
                mask = both(masks, k)
                pull = mask * pull
            u = relaxed(both(ur, k), keep, pull * splat(coef[5, k], p.shape))
            v = relaxed(both(vr, k), keep, pull * splat(coef[6, k], p.shape))
            u = u - (p - both(pr, k, 7))
            v = v - (p - pltpu.roll(p, 1, 1))
            if masked:
                u, v = mask * u, mask * v
            else:
                far = both(domain, 0, 24, 8) * u[24:32]
                u = jnp.concatenate([u[0:24], far], axis=0)
                far = domain[0, 1] * v[:, 128:256]
                v = jnp.concatenate([v[:, 0:128], far], axis=1)
            put(us, k, u)
            put(vs, k, v)

        def down(k, carry, masked):
            q_above, d_above = carry
            if final:
                u, u_east = us[k, 0, 8:24, :], us[k, 0, 9:25, :]
                v_all = both(vs, k, 8, 16)
                v, v_north = v_all[:, 0:128], pltpu.roll(v_all, 255, 1)[:, 0:128]
                p, w = pr[k, 0, 16:32, :], wr[k, 0, 8:24, :]
            else:
                u, u_east = both(us, k), both(us, k, 1)
                v = both(vs, k)
                v_north = pltpu.roll(v, 255, 1)
                p, w = both(pr, k, 8), both(wr, k)

            def level(n):
                return splat(coef[n, k], p.shape)

            divergence = (u_east - u) + (v_north - v)
            q = p - level(4) * divergence
            d = (w - (q_above - q)) * level(0) + level(1) * d_above
            if masked:
                mask = masks[k, 0, 8:24, :] if final else both(masks, k)
                d = mask * d
            if final:
                keep, pull = domain[1, 0, 8:24, :], domain[2, 0, 8:24, :]
                if masked:
                    pull = mask * pull
                uo[k] = keep * u + pull * level(5)
                vo[k] = keep * v + pull * level(6)
                qs[k, 0, 8:24, :] = q
                ds[k, 0, 8:24, :] = d
            else:
                put(qs, k, q)
                put(ds, k, d)
            return q, d

        def each_face(k, carry, masked):
            faces(k, masked)
            return carry

        lax.fori_loop(0, WET_FROM, lambda k, c: each_face(k, c, True), 0, unroll=UF)
        lax.fori_loop(WET_FROM, nz, lambda k, c: each_face(k, c, False), 0, unroll=56)
        zero = jnp.zeros((16, 128) if final else (32, 256), f32)
        carry = lax.fori_loop(
            0, nz - WET_FROM, lambda t, c: down(nz - 1 - t, c, False), (zero, zero), unroll=56
        )
        lax.fori_loop(
            0, WET_FROM, lambda t, c: down(WET_FROM - 1 - t, c, True), carry, unroll=UD
        )

        def up(k, below, masked):
            def level(n):
                return splat(coef[n, k], below.shape)

            if final:
                d, q = ds[k, 0, 8:24, :], qs[k, 0, 8:24, :]
                keep = domain[1, 0, 8:24, :]
            else:
                d, q, keep = both(ds, k), both(qs, k), both(domain, 1)
            w = d + level(2) * below
            p = q - level(3) * (w - below)
            if masked:
                p = (masks[k, 0, 8:24, :] if final else both(masks, k)) * p
            if final:
                wo[k] = (1.0 / H) * (keep * w)
                po[k] = (1.0 / H) * (keep * p)
            else:
                put(ws, k, keep * w)
                put(ps, k, keep * p, 8)
            return w

        below = lax.fori_loop(0, WET_FROM, lambda k, c: up(k, c, True), zero, unroll=8)
        lax.fori_loop(WET_FROM, nz, lambda k, c: up(k, c, False), below, unroll=8)


def neighbours(axis, by):
    size = lax.axis_size(axis)
    return [(i, i + by) for i in range(size) if 0 <= i + by < size]


def send(value, axis, by):
    return lax.ppermute(value, axis, neighbours(axis, by))


def on_device(u, v, w, p, terrain, zones, stiff, inflow):
    nz = u.shape[0]
    groups = nz // 8

    def room(mib):
        return pltpu.CompilerParams(vmem_limit_bytes=mib * 1024 * 1024)


    def arr(*shape):
        return jax.ShapeDtypeStruct(shape, f32)

    hbm = pl.BlockSpec(memory_space=pltpu.HBM)
    in_hbm = [pltpu.with_memory_space_constraint(x, pltpu.HBM) for x in (u, v, w, p, terrain)]
    ylo, yhi, uw, ue = pl.pallas_call(
        pack_a_kernel,
        out_shape=(arr(4 * groups + 1, 16, 128),) * 2 + (arr(2 * nz, 8, 128),) * 2,
        in_specs=[hbm] * 5,
        out_specs=(vmem(),) * 4,
        scratch_shapes=[pltpu.VMEM((nz, 16, 128), f32)] * 4
        + [pltpu.SemaphoreType.DMA((4, 2))]
        + [pltpu.VMEM((16, 128), jnp.int32), pltpu.SemaphoreType.DMA(())],
        compiler_params=room(8),
        name="pack_a",
    )(*in_hbm)
    north = send(ylo, "gy", -1)
    south = send(yhi, "gy", 1)
    ue_in, uw_in = send(uw, "gx", -1), send(ue, "gx", 1)

    def slabs(x):
        return pl.pallas_call(
            pack_b_kernel,
            out_shape=(arr(nz, 8, 128),) * 2,
            in_specs=[vmem()],
            out_specs=(vmem(),) * 2,
            compiler_params=room(4),
        )(x)

    ww, we = slabs(w)
    we_in, ww_in = send(ww, "gx", -1), send(we, "gx", 1)
    pw, pe = slabs(p)
    pe_in, pw_in = send(pw, "gx", -1), send(pe, "gx", 1)
    cw, ce = pl.pallas_call(
        pack_c_kernel,
        out_shape=(arr(6 * groups + 2, 8, 128), arr(5 * groups + 2, 8, 128)),
        in_specs=[vmem()] * 5,
        out_specs=(vmem(),) * 2,
        compiler_params=room(4),
        name="pack_c",
    )(u, p, terrain, north, south)
    ce_in, cw_in = send(cw, "gx", -1), send(ce, "gx", 1)
    prepare = pl.pallas_call(
        functools.partial(prepare_kernel, block=u.shape[1:], nz=nz),
        out_shape=(arr(7, nz, 8, 128), arr(3, 2, 32, 128)),
        in_specs=[smem()] * 3,
        out_specs=(vmem(),) * 2,
        compiler_params=room(8),
        name="prepare",
    )
    coef, domain = prepare(stiff, inflow, zones)
    band = band_matrix()
    advect_uv = pl.pallas_call(
        advect_uv_kernel,
        out_shape=(arr(nz, 48, 128),)
        + (arr(nz, 2, 32, 128),) * 3
        + (arr(WET_FROM + 1, 2, 32, 128),),
        in_specs=[vmem()] * 11,
        out_specs=(vmem(),) * 5,
        scratch_shapes=advect_scratch(8, 64),
        compiler_params=room(20),
        name="advect_uv",
    )
    xu, xv, au, av, masks = advect_uv(
        u, v, terrain, domain, north, south, cw_in, ce_in, uw_in, ue_in, band
    )

    def advect_one(x, f, west, east):
        def kernel(*refs):
            advect_one_kernel(*refs, f=f)

        return pl.pallas_call(
            kernel,
            out_shape=arr(nz, 2, 40 if f == 3 else 32, 128),
            in_specs=[vmem()] * 11,
            out_specs=vmem(),
            scratch_shapes=advect_scratch(16, 16),
            compiler_params=room(16),
            name="advect_w" if f == 2 else "advect_p",
        )(x, xu, xv, masks, north, south, cw_in, ce_in, west, east, band)

    aw = advect_one(w, 2, ww_in, we_in)
    ap = advect_one(p, 3, pw_in, pe_in)
    out = arr(nz, 16, 128)
    return pl.pallas_call(
        substeps_kernel,
        out_shape=(out,) * 4,
        in_specs=[vmem()] * 7,
        out_specs=(vmem(),) * 4,
        scratch_shapes=[
            pltpu.VMEM((nz, 2, rows, 128), f32) for rows in (40, 32, 32, 40, 32, 32)
        ],
        compiler_params=room(34),
        name="substeps",
    )(au, av, aw, ap, masks, domain, coef)


def solution(mesh):
    field = P(None, "gx", "gy")
    return jax.shard_map(
        on_device,
        mesh=mesh,
        in_specs=(field, field, field, field, P("gx", "gy"), P(), P(), P()),
        out_specs=(field, field, field, field),
        check_vma=False,
    )
```
